32 devices in a mesh: rep: 4 (over x, y), pp: 8 (over z, core).
Axes of the slice: x: 2, y: 2, z: 4, core: 2. Of those that a mesh axis runs over, the one named last changes fastest.
Arguments:
- x: bfloat16 [64, 512, 512], P('rep'), parts along dimension 0
- dy: bfloat16 [64, 512, 512], P('rep'), parts along dimension 0
- w_gate: bfloat16 [8, 512, 1536], P('pp')
- w_up: bfloat16 [8, 512, 1536], P('pp')
- w_down: bfloat16 [8, 1536, 512], P('pp')
Outputs:
- output 1: bfloat16 [32, 512, 1536], P(('rep', 'pp')), parts along dimension 0
- output 2: bfloat16 [32, 512, 1536], P(('rep', 'pp')), parts along dimension 0
- output 3: bfloat16 [32, 1536, 512], P(('rep', 'pp')), parts along dimension 0
There are 4 independent parts. The reference program is written for one: setup_inputs(seed, part) draws one part's arguments, and reference() takes and returns one part's arrays. A program takes and returns all parts, laid end to end along the dimension named above; an argument that names none is the same for every part.
All inputs are finite; a program needn't handle non-finite values.
Results may differ from the reference program's by a relative error of at most 0.0282.
Values are sent between devices in bfloat16 or wider.
A program may use at most 2 GiB of HBM per device.

```python
import jax
import jax.numpy as jnp
from jax import lax

MICRO = 16
TOKENS = 512
D = 512
FF = 1536
LAYERS = 8
NAMES = ("w_gate", "w_up", "w_down")
SHAPES = {"w_gate": (LAYERS, D, FF), "w_up": (LAYERS, D, FF), "w_down": (LAYERS, FF, D)}


def bump(key, n, height):
    away = (jnp.arange(n, dtype=jnp.int32) - jax.random.randint(key, (), 0, n, jnp.int32)) % n
    return jnp.where(away < n // 8, height, 1.0)


def together(key, own, strength):
    shared = jax.random.normal(key, own.shape[1:], jnp.float32)
    return (own + strength * shared) * lax.rsqrt(1 + strength * strength)


def setup_inputs(seed: int = 0, part: int = 0) -> dict:
    kx, kdy, ka, kb, kz, kf, kh, kl, *kw = jax.random.split(jax.random.key(seed), 8 + len(NAMES))
    kx, kdy, ka, kb = (jax.random.fold_in(k, part) for k in (kx, kdy, ka, kb))
    shape = (MICRO, TOKENS, D)
    much_x, much_dy = jax.random.uniform(kz, (2,), jnp.float32, 0.0, 1.0)
    layers = 2.0 ** jax.random.uniform(kl, (LAYERS, 1, 1), jnp.float32, -1.0, 1.0)
    x = together(ka, jax.random.normal(kx, shape, jnp.float32), much_x) * bump(kf, D, 4.0)
    dy = together(kb, jax.random.normal(kdy, shape, jnp.float32), much_dy)
    drawn = {"x": x.astype(jnp.bfloat16), "dy": (dy * (MICRO * TOKENS) ** -0.5).astype(jnp.bfloat16)}
    for key, name in zip(kw, NAMES, strict=True):
        w = jax.random.normal(key, SHAPES[name], jnp.float32) * SHAPES[name][1] ** -0.5
        drawn[name] = (w * {"w_gate": 1.0, "w_up": bump(kh, FF, 4.0), "w_down": layers}[name]).astype(jnp.bfloat16)
    return drawn


def matmul(a, w):
    return jnp.dot(a, w, preferred_element_type=jnp.float32).astype(jnp.bfloat16)


def normed(h):
    wide = h.astype(jnp.float32)
    scale = lax.rsqrt(jnp.mean(wide**2, -1, keepdims=True) + 1e-6)
    return (wide * scale).astype(jnp.bfloat16)


def layer(h, w):
    a = normed(h)
    gate = jnp.dot(a, w["w_gate"], preferred_element_type=jnp.float32)
    up = jnp.dot(a, w["w_up"], preferred_element_type=jnp.float32)
    return h + matmul((jax.nn.silu(gate) * up).astype(jnp.bfloat16), w["w_down"])


def stack(weights, h):
    return lax.scan(lambda h, w: (layer(h, w), None), h, weights)[0]


def reference(x, dy, w_gate, w_up, w_down):
    weights = dict(zip(NAMES, (w_gate, w_up, w_down), strict=True))

    def take(so_far, one):
        h, by_y = one
        _, back = jax.vjp(lambda w: stack(w, h), weights)
        return jax.tree.map(lambda total, term: total + term.astype(jnp.float32), so_far, back(by_y)[0]), None

    none_yet = {name: jnp.zeros(w.shape, jnp.float32) for name, w in weights.items()}
    by_weights, _ = lax.scan(take, none_yet, (x, dy))
    return tuple(by_weights[name].astype(jnp.bfloat16) for name in NAMES)
```

```python
import functools

import jax
import jax.numpy as jnp
from jax import lax
from jax.experimental import pallas as pl
from jax.experimental.pallas import tpu as pltpu
from jax.sharding import PartitionSpec as P

F32, BF16 = jnp.float32, jnp.bfloat16
CUTS = 4
TILE = 512


def dot(a, b):
    return jnp.dot(a, b, preferred_element_type=F32)


def rounded(x):
    return x.astype(BF16).astype(F32)


def scale_of(wide):
    return lax.rsqrt(jnp.mean(wide * wide, -1, keepdims=True) + 1e-6)


def sigmoid(x):
    return 1.0 / (1.0 + jnp.exp(-x))


def kernel(stages, x, dy, w_gate, w_up, w_down, out_gate, out_up, out_down, gu_far,
           wg, wu, wd, wgt, wut, wdt, ahead, behind, send_a, send_b, gu, hid, dgate, dup, at, dyt, tot_g, tot_u, tot_d,
           a_blk, h_blk, sem_w, sem_a, sem_b, sem_sa, sem_sb, sem_far, sem_near, sem_out):
    micro, tokens, width = ahead.shape
    ff = wg.shape[1]
    rows_n = tokens // CUTS
    me = lax.axis_index("pp")
    last = stages - 1
    first_stage, last_stage = me == 0, me == last
    to_go = last - me
    delay = 1 + to_go + to_go // 2

    def rows(c):
        return pl.ds(c * rows_n, rows_n)

    def take_x(k, c):
        return pltpu.make_async_copy(x.at[k, rows(c)], ahead.at[k, rows(c)], sem_a.at[k, c])

    def take_dy(k, c):
        return pltpu.make_async_copy(dy.at[k, rows(c)], behind.at[k, rows(c)], sem_b.at[k, c])

    loads = [pltpu.make_async_copy(src.at[0], dst, sem_w.at[i]) for i, (src, dst) in enumerate(((w_gate, wg), (w_up, wu), (w_down, wd)))]

    @pl.when(first_stage)
    def _():
        for c in range(CUTS):
            take_x(0, c).start()

    for load in loads:
        load.start()

    @pl.when(first_stage)
    def _():
        @pl.loop(1, micro)
        def _(k):
            for c in range(CUTS):
                take_x(k, c).start()

    @pl.when(last_stage)
    def _():
        @pl.loop(0, micro)
        def _(k):
            for c in range(CUTS):
                take_dy(k, c).start()

    barrier = pltpu.get_barrier_semaphore()

    @pl.when(me > 0)
    def _():
        pl.semaphore_signal(barrier, inc=1, device_id={"pp": me - 1}, device_id_type=pl.DeviceIdType.MESH)

    @pl.when(me < last)
    def _():
        pl.semaphore_signal(barrier, inc=1, device_id={"pp": me + 1}, device_id_type=pl.DeviceIdType.MESH)

    pl.semaphore_wait(barrier, jnp.minimum(me, 1) + jnp.minimum(last - me, 1))

    def pass_on(k, c):
        return pltpu.make_async_remote_copy(
            src_ref=send_a.at[k % 2, rows(c)], dst_ref=ahead.at[k, rows(c)], send_sem=sem_sa.at[k % 2, c], recv_sem=sem_a.at[k, c],
            device_id={"pp": jnp.minimum(me + 1, last)}, device_id_type=pl.DeviceIdType.MESH)

    def pass_back(m, c):
        return pltpu.make_async_remote_copy(
            src_ref=send_b.at[m % 2, rows(c)], dst_ref=behind.at[m, rows(c)], send_sem=sem_sb.at[m % 2, c], recv_sem=sem_b.at[m, c],
            device_id={"pp": jnp.maximum(me - 1, 0)}, device_id_type=pl.DeviceIdType.MESH)

    def put_away(k, c):
        return pltpu.make_async_copy(gu.at[c], gu_far.at[k, c], sem_far.at[c])

    def fetch(m, c):
        return pltpu.make_async_copy(gu_far.at[m, c], gu.at[CUTS + c], sem_near.at[c])

    def forward(k):
        for c in range(CUTS):
            take_x(k, c).wait()

            @pl.when((me < last) & (k >= 1))
            def _():
                put_away(k - 1, c).wait()

            wide = ahead[k, rows(c), :].astype(F32)
            a_blk[...] = (wide * scale_of(wide)).astype(BF16)
            for n in range(0, ff, TILE):
                g = dot(a_blk[...], wg[:, n:n + TILE])
                u = dot(a_blk[...], wu[:, n:n + TILE])
                gu[c, :, n:n + TILE] = g
                gu[c, :, ff + n:ff + n + TILE] = u
                h_blk[:, n:n + TILE] = (g * sigmoid(g) * u).astype(BF16)

            @pl.when(me < last)
            def _():
                put_away(k, c).start()

                @pl.when(k >= 2)
                def _():
                    pass_on(k, c).wait_send()

                y = rounded(dot(h_blk[...], wd[...]))
                send_a[k % 2, rows(c), :] = (ahead[k, rows(c), :].astype(F32) + y).astype(BF16)
                pass_on(k, c).start()

    def backward(m):
        base = jnp.where(me < last, CUTS, 0)
        for c in range(CUTS):
            take_dy(m, c).wait()

            @pl.when(me < last)
            def _():
                fetch(m, c).wait()

            for n in range(0, ff, TILE):
                dh = rounded(dot(behind[m, rows(c), :], wdt[:, n:n + TILE]))
                g = gu[base + c, :, n:n + TILE]
                u = gu[base + c, :, ff + n:ff + n + TILE]
                s = sigmoid(g)
                t = g * s
                hid[rows(c), n:n + TILE] = (t * u).astype(BF16)
                dup[rows(c), n:n + TILE] = (dh * t).astype(BF16)
                dgate[rows(c), n:n + TILE] = (dh * u * (s + t * (1.0 - s))).astype(BF16)

            @pl.when(me > 0)
            def _():
                @pl.when(m >= 2)
                def _():
                    pass_back(m, c).wait_send()

                da = rounded(dot(dup[rows(c), :], wut[...])) + rounded(dot(dgate[rows(c), :], wgt[...]))
                da = rounded(da)
                wide = ahead[m, rows(c), :].astype(F32)
                scale = scale_of(wide)
                inner = jnp.sum(da * wide, -1, keepdims=True)
                by_norm = rounded(da * scale + (inner * (scale * scale * scale) * (-1.0 / width)) * wide)
                send_b[m % 2, rows(c), :] = (behind[m, rows(c), :].astype(F32) + by_norm).astype(BF16)
                pass_back(m, c).start()

    def weights(m):
        wide = ahead[m].astype(F32)
        at[...] = (wide * scale_of(wide)).astype(BF16).T
        dyt[...] = behind[m].T
        for n in range(0, ff, TILE):
            tot_g[:, n:n + TILE] += rounded(dot(at[...], dgate[:, n:n + TILE]))
            tot_u[:, n:n + TILE] += rounded(dot(at[...], dup[:, n:n + TILE]))
            tot_d[:, n:n + TILE] += rounded(dot(dyt[...], hid[:, n:n + TILE]))

    for load in loads:
        load.wait()

    @pl.loop(0, micro + delay)
    def _(k):
        m = k - delay

        @pl.when(m >= 0)
        def _():
            backward(m)

        @pl.when(k < micro)
        def _():
            forward(k)

        @pl.when((me < last) & (k == micro))
        def _():
            for c in range(CUTS):
                put_away(micro - 1, c).wait()

        @pl.when((me < last) & (m + 1 >= 0) & (m + 1 < micro))
        def _():
            for c in range(CUTS):
                fetch(m + 1, c).start()

        @pl.when(k == 0)
        def _():
            wdt[...] = wd[...].T
            wgt[...] = wg[...].T
            wut[...] = wu[...].T
            tot_g[...] = jnp.zeros_like(tot_g)
            tot_u[...] = jnp.zeros_like(tot_u)
            tot_d[...] = jnp.zeros_like(tot_d)

        @pl.when(m >= 0)
        def _():
            weights(m)

    dgate[...] = tot_g[...].astype(BF16)
    dup[...] = tot_u[...].astype(BF16)
    hid[...] = tot_d[...].astype(BF16)
    stores = [pltpu.make_async_copy(src, dst.at[0], sem_out.at[i])
              for i, (src, dst) in enumerate(((dgate, out_gate), (dup, out_up), (hid, out_down)))]
    for store in stores:
        store.start()

    @pl.when(me < last)
    def _():
        for k in (micro - 2, micro - 1):
            for c in range(CUTS):
                pass_on(k, c).wait_send()

    @pl.when(me > 0)
    def _():
        for m in (micro - 2, micro - 1):
            for c in range(CUTS):
                pass_back(m, c).wait_send()

    for store in stores:
        store.wait()


def solution(mesh):
    stages = mesh.shape["pp"]

    def step(x, dy, w_gate, w_up, w_down):
        micro, tokens, width = x.shape
        ff = w_gate.shape[2]
        whole = (micro, tokens, width)
        rows_n = tokens // CUTS
        vmem, dma = pltpu.VMEM, pltpu.SemaphoreType.DMA
        any_space = pl.BlockSpec(memory_space=pl.ANY)
        g, u, d, _ = pl.pallas_call(
            functools.partial(kernel, stages),
            out_shape=(jax.ShapeDtypeStruct((1, width, ff), BF16),) * 3
            + (jax.ShapeDtypeStruct((micro, CUTS, rows_n, 2 * ff), F32),),
            in_specs=[any_space] * 5,
            out_specs=(any_space,) * 4,
            scratch_shapes=[
                vmem((width, ff), BF16), vmem((width, ff), BF16), vmem((ff, width), BF16),
                vmem((ff, width), BF16), vmem((ff, width), BF16), vmem((width, ff), BF16),
                vmem(whole, BF16), vmem(whole, BF16),
                vmem((2, tokens, width), BF16), vmem((2, tokens, width), BF16),
                vmem((2 * CUTS, rows_n, 2 * ff), F32),
                vmem((tokens, ff), BF16), vmem((tokens, ff), BF16), vmem((tokens, ff), BF16),
                vmem((width, tokens), BF16), vmem((width, tokens), BF16),
                vmem((width, ff), F32), vmem((width, ff), F32), vmem((width, ff), F32),
                vmem((rows_n, width), BF16), vmem((rows_n, ff), BF16),
                dma((3,)), dma((micro, CUTS)), dma((micro, CUTS)), dma((2, CUTS)), dma((2, CUTS)),
                dma((CUTS,)), dma((CUTS,)), dma((3,)),
            ],
            compiler_params=pltpu.CompilerParams(collective_id=0, has_side_effects=True, vmem_limit_bytes=67_000_000),
            name="pipeline",
        )(x, dy, w_gate, w_up, w_down)
        return g, u, d.transpose(0, 2, 1)

    return jax.shard_map(
        step,
        mesh=mesh,
        in_specs=(P("rep", None, None),) * 2 + (P("pp", None, None),) * 3,
        out_specs=(P(("rep", "pp"), None, None),) * 3,
        check_vma=False,
    )
```

```python
import jax
import jax.numpy as jnp
from jax import lax
from jax.experimental import pallas as pl
from jax.experimental.pallas import tpu as pltpu
from jax.sharding import PartitionSpec as P

F32, BF16 = jnp.float32, jnp.bfloat16
CUTS = 4
TILE = 512


def dot(a, b):
    return jnp.dot(a, b, preferred_element_type=F32)


def rounded(x):
    return x.astype(BF16).astype(F32)


def scale_of(wide):
    return lax.rsqrt(jnp.mean(wide * wide, -1, keepdims=True) + 1e-6)


def kernel(x, dy, w_gate, w_up, w_down, out_gate, out_up, out_down, far_act, far_hid,
           wg, wu, wd, wgt, wut, wdt, ahead, behind, send_a, send_b, act, hidden, dgate, dup, at, dyt, tot_g, tot_u, tot_d,
           a_blk, sem_w, sem_a, sem_b, sem_sa, sem_sb, sem_far, sem_near, sem_hfar, sem_hnear, sem_out):
    micro, tokens, width = ahead.shape
    ff = wg.shape[1]
    rows_n = tokens // CUTS
    me, last = lax.axis_index("pp"), lax.axis_size("pp") - 1
    to_go = last - me
    delay = to_go + to_go // 2
    near = delay == 1

    def rows(c):
        return pl.ds(pl.multiple_of(c * rows_n, rows_n), rows_n)

    def each(f):
        pl.loop(0, CUTS)(f)

    def take_x(k, c):
        return pltpu.make_async_copy(x.at[k, rows(c)], ahead.at[k, rows(c)], sem_a.at[k, c])

    def take_dy(k, c):
        return pltpu.make_async_copy(dy.at[k, rows(c)], behind.at[k, rows(c)], sem_b.at[k, c])

    loads = [pltpu.make_async_copy(src.at[0], dst, sem_w.at[i]) for i, (src, dst) in enumerate(((w_gate, wg), (w_up, wu), (w_down, wd)))]

    @pl.when(me == 0)
    def _():
        each(lambda c: take_x(0, c).start())

    for load in loads:
        load.start()

    @pl.when(me == 0)
    def _():
        @pl.loop(1, micro)
        def _(k):
            each(lambda c: take_x(k, c).start())

    @pl.when(me == last)
    def _():
        @pl.loop(0, micro)
        def _(k):
            each(lambda c: take_dy(k, c).start())

    barrier = pltpu.get_barrier_semaphore()

    @pl.when(me > 0)
    def _():
        pl.semaphore_signal(barrier, inc=1, device_id={"pp": me - 1}, device_id_type=pl.DeviceIdType.MESH)

    @pl.when(me < last)
    def _():
        pl.semaphore_signal(barrier, inc=1, device_id={"pp": me + 1}, device_id_type=pl.DeviceIdType.MESH)

    pl.semaphore_wait(barrier, jnp.minimum(me, 1) + jnp.minimum(last - me, 1))

    def pass_on(k, c):
        return pltpu.make_async_remote_copy(
            src_ref=send_a.at[k % 2, rows(c)], dst_ref=ahead.at[k, rows(c)], send_sem=sem_sa.at[k % 2, c], recv_sem=sem_a.at[k, c],
            device_id={"pp": jnp.minimum(me + 1, last)}, device_id_type=pl.DeviceIdType.MESH)

    def pass_back(m, c):
        return pltpu.make_async_remote_copy(
            src_ref=send_b.at[m % 2, rows(c)], dst_ref=behind.at[m, rows(c)], send_sem=sem_sb.at[m % 2, c], recv_sem=sem_b.at[m, c],
            device_id={"pp": jnp.maximum(me - 1, 0)}, device_id_type=pl.DeviceIdType.MESH)

    def slot_f(k):
        return jnp.where(near, k % 2, 0)

    def slot_b(m):
        return jnp.where(near, m % 2, 1)

    def put_away(k, c):
        return (pltpu.make_async_copy(act.at[0, c], far_act.at[k, c], sem_far.at[c]),
                pltpu.make_async_copy(hidden.at[0, rows(c)], far_hid.at[k, rows(c)], sem_hfar.at[c]))

    def fetch(m, c):
        return pltpu.make_async_copy(far_act.at[m, c], act.at[1, c], sem_near.at[c])

    def fetch_hidden(m):
        return pltpu.make_async_copy(far_hid.at[m], hidden.at[1], sem_hnear.at[0])

    def silu_parts(g, u):
        half = 0.5 * g
        z = jnp.tanh(half)
        q = half * z
        return half + q, u * ((0.5 * z + 0.5) * ((half - q) + 1.0))

    def work_forward(k, c):
        slot = slot_f(k)
        wide = ahead[k, rows(c), :].astype(F32)
        a_blk[...] = (wide * scale_of(wide)).astype(BF16)
        for n in range(0, ff, TILE):
            g = dot(a_blk[...], wg[:, n:n + TILE])
            u = dot(a_blk[...], wu[:, n:n + TILE])
            t, v = silu_parts(g, u)
            act[slot, c, :, n:n + TILE] = t
            act[slot, c, :, ff + n:ff + n + TILE] = v
            hidden[slot, rows(c), n:n + TILE] = (t * u).astype(BF16)
        y = rounded(dot(hidden[slot, rows(c), :], wd[...]))
        send_a[k % 2, rows(c), :] = (ahead[k, rows(c), :].astype(F32) + y).astype(BF16)

    def by_hidden(m, c):
        slot = slot_b(m)
        for n in range(0, ff, TILE):
            dh = rounded(dot(behind[m, rows(c), :], wdt[:, n:n + TILE]))
            dup[rows(c), n:n + TILE] = (dh * act[slot, c, :, n:n + TILE]).astype(BF16)
            dgate[rows(c), n:n + TILE] = (dh * act[slot, c, :, ff + n:ff + n + TILE]).astype(BF16)

    def by_input(m, c):
        da = rounded(rounded(dot(dup[rows(c), :], wut[...])) + rounded(dot(dgate[rows(c), :], wgt[...])))
        wide = ahead[m, rows(c), :].astype(F32)
        scale = scale_of(wide)
        inner = jnp.sum(da * wide, -1, keepdims=True)
        by_norm = rounded(da * scale + (inner * (scale * scale * scale) * (-1.0 / width)) * wide)
        send_b[m % 2, rows(c), :] = (behind[m, rows(c), :].astype(F32) + by_norm).astype(BF16)

    def work_last(k, c):
        wide = ahead[k, rows(c), :].astype(F32)
        a_blk[...] = (wide * scale_of(wide)).astype(BF16)
        for n in range(0, ff, TILE):
            g = dot(a_blk[...], wg[:, n:n + TILE])
            u = dot(a_blk[...], wu[:, n:n + TILE])
            dh = rounded(dot(behind[k, rows(c), :], wdt[:, n:n + TILE]))
            t, v = silu_parts(g, u)
            hidden[0, rows(c), n:n + TILE] = (t * u).astype(BF16)
            dup[rows(c), n:n + TILE] = (dh * t).astype(BF16)
            dgate[rows(c), n:n + TILE] = (dh * v).astype(BF16)
        by_input(k, c)

    def weights(m, slot):
        wide = ahead[m].astype(F32)
        at[...] = (wide * scale_of(wide)).astype(BF16).T
        dyt[...] = behind[m].T
        for n in range(0, ff, TILE):
            tot_g[:, n:n + TILE] += rounded(dot(at[...], dgate[:, n:n + TILE]))
            tot_u[:, n:n + TILE] += rounded(dot(at[...], dup[:, n:n + TILE]))
            tot_d[:, n:n + TILE] += rounded(dot(dyt[...], hidden[slot, :, n:n + TILE]))

    def before_forward(k, c):
        take_x(k, c).wait()

        @pl.when((k >= 1) & ~near)
        def _():
            for copy in put_away(k - 1, c):
                copy.wait()

        @pl.when(k >= 2)
        def _():
            pass_on(k, c).wait_send()

    def after_forward(k, c):
        pass_on(k, c).start()

        @pl.when(~near)
        def _():
            for copy in put_away(k, c):
                copy.start()

    def before_backward(m, c, send):
        take_dy(m, c).wait()

        @pl.when(~near)
        def _():
            fetch(m, c).wait()

        if send:
            @pl.when(m >= 2)
            def _():
                pass_back(m, c).wait_send()

    def turn():
        wdt[...] = wd[...].T
        wgt[...] = wg[...].T
        wut[...] = wu[...].T

    def clear():
        tot_g[...] = jnp.zeros_like(tot_g)
        tot_u[...] = jnp.zeros_like(tot_u)
        tot_d[...] = jnp.zeros_like(tot_d)

    def run(send):
        @pl.loop(0, micro + delay)
        def _(k):
            m = k - delay

            @pl.when(m < 0)
            def _():
                @each
                def _(c):
                    before_forward(k, c)
                    work_forward(k, c)
                    after_forward(k, c)

            @pl.when((m >= 0) & (k < micro))
            def _():
                @each
                def _(c):
                    before_backward(m, c, send)
                    before_forward(k, c)
                    work_forward(k, c)
                    by_hidden(m, c)
                    if send:
                        by_input(m, c)
                        pass_back(m, c).start()
                    after_forward(k, c)

            @pl.when(k >= micro)
            def _():
                @each
                def _(c):
                    before_backward(m, c, send)
                    by_hidden(m, c)
                    if send:
                        by_input(m, c)
                        pass_back(m, c).start()

            @pl.when((k == micro) & ~near)
            def _():
                @each
                def _(c):
                    for copy in put_away(micro - 1, c):
                        copy.wait()

            coming = (m + 1 >= 0) & (m + 1 < micro) & ~near

            @pl.when(coming)
            def _():
                each(lambda c: fetch(m + 1, c).start())

            @pl.when(k == 0)
            def _():
                turn()
                clear()

            @pl.when(m >= 0)
            def _():
                @pl.when(~near)
                def _():
                    fetch_hidden(m).wait()

                weights(m, slot_b(m))

            @pl.when(coming)
            def _():
                fetch_hidden(m + 1).start()

    for load in loads:
        load.wait()

    @pl.when(me == 0)
    def _():
        run(False)

    @pl.when((me > 0) & (me < last))
    def _():
        run(True)

    @pl.when(me == last)
    def _():
        turn()
        clear()

        @pl.loop(0, micro)
        def _(k):
            @each
            def _(c):
                take_x(k, c).wait()
                take_dy(k, c).wait()

                @pl.when(k >= 2)
                def _():
                    pass_back(k, c).wait_send()

                work_last(k, c)
                pass_back(k, c).start()

            weights(k, 0)

    dgate[...] = tot_g[...].astype(BF16)
    stores = [pltpu.make_async_copy(src, dst.at[0], sem_out.at[i])
              for i, (src, dst) in enumerate(((dgate, out_gate), (dup, out_up), (wd, out_down)))]
    stores[0].start()
    dup[...] = tot_u[...].astype(BF16)
    stores[1].start()
    wd[...] = tot_d[...].astype(BF16).T
    stores[2].start()

    @pl.when(me < last)
    def _():
        for k in (micro - 2, micro - 1):
            each(lambda c, k=k: pass_on(k, c).wait_send())

    @pl.when(me > 0)
    def _():
        for m in (micro - 2, micro - 1):
            each(lambda c, m=m: pass_back(m, c).wait_send())

    for store in stores:
        store.wait()


def solution(mesh):
    def step(x, dy, w_gate, w_up, w_down):
        micro, tokens, width = x.shape
        ff = w_gate.shape[2]
        rows_n = tokens // CUTS
        vmem, dma = pltpu.VMEM, pltpu.SemaphoreType.DMA
        any_space = pl.BlockSpec(memory_space=pl.ANY)
        g, u, d, _, _ = pl.pallas_call(
            kernel,
            out_shape=(
                jax.ShapeDtypeStruct((1, width, ff), BF16), jax.ShapeDtypeStruct((1, width, ff), BF16),
                jax.ShapeDtypeStruct((1, ff, width), BF16),
                jax.ShapeDtypeStruct((micro, CUTS, rows_n, 2 * ff), F32), jax.ShapeDtypeStruct((micro, tokens, ff), BF16)),
            in_specs=[any_space] * 5,
            out_specs=(any_space,) * 5,
            scratch_shapes=[
                vmem((width, ff), BF16), vmem((width, ff), BF16), vmem((ff, width), BF16),
                vmem((ff, width), BF16), vmem((ff, width), BF16), vmem((width, ff), BF16),
                vmem(x.shape, BF16), vmem(x.shape, BF16),
                vmem((2, tokens, width), BF16), vmem((2, tokens, width), BF16),
                vmem((2, CUTS, rows_n, 2 * ff), F32), vmem((2, tokens, ff), BF16),
                vmem((tokens, ff), BF16), vmem((tokens, ff), BF16),
                vmem((width, tokens), BF16), vmem((width, tokens), BF16),
                vmem((width, ff), F32), vmem((width, ff), F32), vmem((width, ff), F32),
                vmem((rows_n, width), BF16),
                dma((3,)), dma((micro, CUTS)), dma((micro, CUTS)), dma((2, CUTS)), dma((2, CUTS)),
                dma((CUTS,)), dma((CUTS,)), dma((CUTS,)), dma((1,)), dma((3,)),
            ],
            compiler_params=pltpu.CompilerParams(collective_id=0, has_side_effects=True, vmem_limit_bytes=67_000_000),
            name="pipeline",
        )(x, dy, w_gate, w_up, w_down)
        return g, u, d

    return jax.shard_map(
        step,
        mesh=mesh,
        in_specs=(P("rep", None, None),) * 2 + (P("pp", None, None),) * 3,
        out_specs=(P(("rep", "pp"), None, None),) * 3,
        check_vma=False,
    )
```

```python
import jax
import jax.numpy as jnp
from jax import lax
from jax.experimental import pallas as pl
from jax.experimental.pallas import tpu as pltpu
from jax.sharding import PartitionSpec as P

F32, BF16 = jnp.float32, jnp.bfloat16
CUTS = 4
TILE = 512


def dot(a, b):
    return jnp.dot(a, b, preferred_element_type=F32)


def rounded(x):
    return x.astype(BF16).astype(F32)


def scale_of(wide):
    return lax.rsqrt(jnp.mean(wide * wide, -1, keepdims=True) + 1e-6)


def kernel(x, dy, w_gate, w_up, w_down, out_gate, out_up, out_down, far_act, far_hid,
           wg, wu, wd, wgt, wut, wdt, ahead, behind, send_a, send_b, act, hidden, dgate, dup, at, dyt, tot_g, tot_u, tot_d,
           a_blk, sem_w, sem_a, sem_b, sem_sa, sem_sb, sem_far, sem_near, sem_hfar, sem_hnear, sem_out):
    micro, tokens, width = ahead.shape
    ff = wg.shape[1]
    rows_n = tokens // CUTS
    me, last = lax.axis_index("pp"), lax.axis_size("pp") - 1
    to_go = last - me
    delay = to_go + to_go // 2
    near = delay == 1

    def rows(c):
        return pl.ds(pl.multiple_of(c * rows_n, rows_n), rows_n)

    def each(f):
        pl.loop(0, CUTS)(f)

    def take_x(k, c):
        return pltpu.make_async_copy(x.at[k, rows(c)], ahead.at[k, rows(c)], sem_a.at[k, c])

    def take_dy(k, c):
        return pltpu.make_async_copy(dy.at[k, rows(c)], behind.at[k, rows(c)], sem_b.at[k, c])

    loads = [pltpu.make_async_copy(src.at[0], dst, sem_w.at[i]) for i, (src, dst) in enumerate(((w_gate, wg), (w_up, wu), (w_down, wd)))]

    @pl.when(me == 0)
    def _():
        each(lambda c: take_x(0, c).start())

    for load in loads:
        load.start()

    @pl.when(me == 0)
    def _():
        @pl.loop(1, micro)
        def _(k):
            each(lambda c: take_x(k, c).start())

    @pl.when(me == last)
    def _():
        @pl.loop(0, micro)
        def _(k):
            each(lambda c: take_dy(k, c).start())

    barrier = pltpu.get_barrier_semaphore()

    @pl.when(me > 0)
    def _():
        pl.semaphore_signal(barrier, inc=1, device_id={"pp": me - 1}, device_id_type=pl.DeviceIdType.MESH)

    @pl.when(me < last)
    def _():
        pl.semaphore_signal(barrier, inc=1, device_id={"pp": me + 1}, device_id_type=pl.DeviceIdType.MESH)

    pl.semaphore_wait(barrier, jnp.minimum(me, 1) + jnp.minimum(last - me, 1))

    def pass_on(k, c):
        return pltpu.make_async_remote_copy(
            src_ref=send_a.at[k % 2, rows(c)], dst_ref=ahead.at[k, rows(c)], send_sem=sem_sa.at[k % 2, c], recv_sem=sem_a.at[k, c],
            device_id={"pp": jnp.minimum(me + 1, last)}, device_id_type=pl.DeviceIdType.MESH)

    def pass_back(m, c):
        return pltpu.make_async_remote_copy(
            src_ref=send_b.at[m % 2, rows(c)], dst_ref=behind.at[m, rows(c)], send_sem=sem_sb.at[m % 2, c], recv_sem=sem_b.at[m, c],
            device_id={"pp": jnp.maximum(me - 1, 0)}, device_id_type=pl.DeviceIdType.MESH)

    def slot_f(k):
        return jnp.where(near, k % 2, 0)

    def slot_b(m):
        return jnp.where(near, m % 2, 1)

    def hidden_f(k):
        return jnp.where(near, k % 3, 0)

    def hidden_w(m):
        return jnp.where(near, m % 3, 1 + m % 2)

    def put_away(k, c):
        return (pltpu.make_async_copy(act.at[0, c], far_act.at[k, c], sem_far.at[c]),
                pltpu.make_async_copy(hidden.at[0, rows(c)], far_hid.at[k, rows(c)], sem_hfar.at[c]))

    def fetch(m, c):
        return pltpu.make_async_copy(far_act.at[m, c], act.at[1, c], sem_near.at[c])

    def fetch_hidden(m):
        return pltpu.make_async_copy(far_hid.at[m], hidden.at[1 + m % 2], sem_hnear.at[m % 2])

    def silu_parts(g, u):
        half = 0.5 * g
        z = jnp.tanh(half)
        q = half * z
        return half + q, u * ((0.5 * z + 0.5) * ((half - q) + 1.0))

    def work_forward(k, c):
        slot, slot_h = slot_f(k), hidden_f(k)
        wide = ahead[k, rows(c), :].astype(F32)
        a_blk[...] = (wide * scale_of(wide)).astype(BF16)
        for n in range(0, ff, TILE):
            g = dot(a_blk[...], wg[:, n:n + TILE])
            u = dot(a_blk[...], wu[:, n:n + TILE])
            t, v = silu_parts(g, u)
            act[slot, c, :, n:n + TILE] = t
            act[slot, c, :, ff + n:ff + n + TILE] = v
            hidden[slot_h, rows(c), n:n + TILE] = (t * u).astype(BF16)
        y = rounded(dot(hidden[slot_h, rows(c), :], wd[...]))
        send_a[k % 2, rows(c), :] = (ahead[k, rows(c), :].astype(F32) + y).astype(BF16)

    def by_hidden(m, c):
        slot, keep = slot_b(m), m % 2
        for n in range(0, ff, TILE):
            dh = rounded(dot(behind[m, rows(c), :], wdt[:, n:n + TILE]))
            dup[keep, rows(c), n:n + TILE] = (dh * act[slot, c, :, n:n + TILE]).astype(BF16)
            dgate[keep, rows(c), n:n + TILE] = (dh * act[slot, c, :, ff + n:ff + n + TILE]).astype(BF16)

    def by_input(m, c, keep, send):
        if send:
            da = rounded(rounded(dot(dup[keep, rows(c), :], wut[...])) + rounded(dot(dgate[keep, rows(c), :], wgt[...])))
        wide = ahead[m, rows(c), :].astype(F32)
        scale = scale_of(wide)
        normed = wide * scale
        at[keep, :, rows(c)] = normed.astype(BF16).T
        dyt[keep, :, rows(c)] = behind[m, rows(c), :].T
        if send:
            inner = jnp.sum(da * wide, -1, keepdims=True)
            by_norm = rounded(da * scale + (inner * (scale * scale * scale) * (-1.0 / width)) * wide)
            send_b[m % 2, rows(c), :] = (behind[m, rows(c), :].astype(F32) + by_norm).astype(BF16)

    def work_last(k, c):
        wide = ahead[k, rows(c), :].astype(F32)
        a_blk[...] = (wide * scale_of(wide)).astype(BF16)
        for n in range(0, ff, TILE):
            g = dot(a_blk[...], wg[:, n:n + TILE])
            u = dot(a_blk[...], wu[:, n:n + TILE])
            dh = rounded(dot(behind[k, rows(c), :], wdt[:, n:n + TILE]))
            t, v = silu_parts(g, u)
            hidden[k % 2, rows(c), n:n + TILE] = (t * u).astype(BF16)
            dup[k % 2, rows(c), n:n + TILE] = (dh * t).astype(BF16)
            dgate[k % 2, rows(c), n:n + TILE] = (dh * v).astype(BF16)
        by_input(k, c, k % 2, True)

    def weights(keep, slot):
        for n in range(0, ff, TILE):
            tot_g[:, n:n + TILE] += rounded(dot(at[keep], dgate[keep, :, n:n + TILE]))
            tot_u[:, n:n + TILE] += rounded(dot(at[keep], dup[keep, :, n:n + TILE]))
            tot_d[:, n:n + TILE] += rounded(dot(dyt[keep], hidden[slot, :, n:n + TILE]))

    def weights_part(keep, slot, c):
        part = pl.ds(pl.multiple_of(c * (width // CUTS), width // CUTS), width // CUTS)
        tot_g[part, :] += rounded(dot(at[keep, part, :], dgate[keep]))
        tot_u[part, :] += rounded(dot(at[keep, part, :], dup[keep]))
        tot_d[part, :] += rounded(dot(dyt[keep, part, :], hidden[slot]))

    def before_forward(k, c):
        take_x(k, c).wait()

        @pl.when((k >= 1) & ~near)
        def _():
            for copy in put_away(k - 1, c):
                copy.wait()

        @pl.when(k >= 2)
        def _():
            pass_on(k, c).wait_send()

    def after_forward(k, c):
        pass_on(k, c).start()

        @pl.when(~near)
        def _():
            for copy in put_away(k, c):
                copy.start()

    def before_backward(m, c, send):
        take_dy(m, c).wait()

        @pl.when(~near)
        def _():
            fetch(m, c).wait()

        if send:
            @pl.when(m >= 2)
            def _():
                pass_back(m, c).wait_send()

    def turn():
        wdt[...] = wd[...].T
        wgt[...] = wg[...].T
        wut[...] = wu[...].T

    def clear():
        tot_g[...] = jnp.zeros_like(tot_g)
        tot_u[...] = jnp.zeros_like(tot_u)
        tot_d[...] = jnp.zeros_like(tot_d)

    def run(send):
        @pl.loop(0, micro + delay)
        def _(k):
            m = k - delay

            @pl.when(m < 0)
            def _():
                @each
                def _(c):
                    before_forward(k, c)
                    work_forward(k, c)
                    after_forward(k, c)

            @pl.when((m >= 0) & (m < micro) & ~near)
            def _():
                fetch_hidden(m).start()

            @pl.when((m >= 1) & ~near)
            def _():
                fetch_hidden(m - 1).wait()

            def fetch_next(c):
                @pl.when((m + 1 < micro) & ~near)
                def _():
                    fetch(m + 1, c).start()

            def both(c):
                before_backward(m, c, send)
                before_forward(k, c)
                work_forward(k, c)
                by_hidden(m, c)
                by_input(m, c, m % 2, send)

            def both_sent(c):
                if send:
                    pass_back(m, c).start()
                after_forward(k, c)
                fetch_next(c)

            @pl.when(m == 0)
            def _():
                @each
                def _(c):
                    both(c)
                    both_sent(c)

            @pl.when((m >= 1) & (k < micro))
            def _():
                keep, slot = (m - 1) % 2, hidden_w(m - 1)

                @each
                def _(c):
                    both(c)
                    weights_part(keep, slot, c)
                    both_sent(c)

            @pl.when((k == micro) & ~near)
            def _():
                @each
                def _(c):
                    for copy in put_away(micro - 1, c):
                        copy.wait()

            @pl.when(k >= micro)
            def _():
                weights((m - 1) % 2, hidden_w(m - 1))

                @each
                def _(c):
                    before_backward(m, c, send)
                    by_hidden(m, c)
                    by_input(m, c, m % 2, send)
                    if send:
                        pass_back(m, c).start()
                    fetch_next(c)

            @pl.when((m == -1) & ~near)
            def _():
                each(lambda c: fetch(0, c).start())

            @pl.when(k == 0)
            def _():
                turn()
                clear()

    for load in loads:
        load.wait()

    @pl.when(me == 0)
    def _():
        run(False)

    @pl.when((me > 0) & (me < last))
    def _():
        run(True)

    @pl.when(me == last)
    def _():
        turn()
        clear()

        def block(k, c, part):
            take_x(k, c).wait()
            take_dy(k, c).wait()

            @pl.when(k >= 2)
            def _():
                pass_back(k, c).wait_send()

            work_last(k, c)
            if part:
                weights_part((k - 1) % 2, (k - 1) % 2, c)
            pass_back(k, c).start()

        each(lambda c: block(0, c, False))

        @pl.loop(1, micro)
        def _(k):
            each(lambda c: block(k, c, True))

    @pl.when((me < last) & ~near)
    def _():
        fetch_hidden(micro - 1).wait()

    keep = (micro - 1) % 2
    spare = 1 - keep
    slot = jnp.where(me == last, keep, hidden_w(micro - 1))
    stores = [pltpu.make_async_copy(src, dst.at[0], sem_out.at[i])
              for i, (src, dst) in enumerate(((dgate.at[spare], out_gate), (dup.at[spare], out_up), (wd, out_down)))]
    for n in range(0, ff, TILE):
        dgate[spare, :, n:n + TILE] = (tot_g[:, n:n + TILE] + rounded(dot(at[keep], dgate[keep, :, n:n + TILE]))).astype(BF16)
    stores[0].start()
    for n in range(0, ff, TILE):
        dup[spare, :, n:n + TILE] = (tot_u[:, n:n + TILE] + rounded(dot(at[keep], dup[keep, :, n:n + TILE]))).astype(BF16)
    stores[1].start()
    for n in range(0, ff, TILE):
        wd[n:n + TILE, :] = (tot_d[:, n:n + TILE] + rounded(dot(dyt[keep], hidden[slot, :, n:n + TILE]))).astype(BF16).T
    stores[2].start()

    @pl.when(me < last)
    def _():
        for k in (micro - 2, micro - 1):
            each(lambda c, k=k: pass_on(k, c).wait_send())

    @pl.when(me > 0)
    def _():
        for m in (micro - 2, micro - 1):
            each(lambda c, m=m: pass_back(m, c).wait_send())

    for store in stores:
        store.wait()


def solution(mesh):
    def step(x, dy, w_gate, w_up, w_down):
        micro, tokens, width = x.shape
        ff = w_gate.shape[2]
        rows_n = tokens // CUTS
        vmem, dma = pltpu.VMEM, pltpu.SemaphoreType.DMA
        any_space = pl.BlockSpec(memory_space=pl.ANY)
        g, u, d, _, _ = pl.pallas_call(
            kernel,
            out_shape=(
                jax.ShapeDtypeStruct((1, width, ff), BF16), jax.ShapeDtypeStruct((1, width, ff), BF16),
                jax.ShapeDtypeStruct((1, ff, width), BF16),
                jax.ShapeDtypeStruct((micro, CUTS, rows_n, 2 * ff), F32), jax.ShapeDtypeStruct((micro, tokens, ff), BF16)),
            in_specs=[any_space] * 5,
            out_specs=(any_space,) * 5,
            scratch_shapes=[
                vmem((width, ff), BF16), vmem((width, ff), BF16), vmem((ff, width), BF16),
                vmem((ff, width), BF16), vmem((ff, width), BF16), vmem((width, ff), BF16),
                vmem(x.shape, BF16), vmem(x.shape, BF16),
                vmem((2, tokens, width), BF16), vmem((2, tokens, width), BF16),
                vmem((2, CUTS, rows_n, 2 * ff), F32), vmem((3, tokens, ff), BF16),
                vmem((2, tokens, ff), BF16), vmem((2, tokens, ff), BF16),
                vmem((2, width, tokens), BF16), vmem((2, width, tokens), BF16),
                vmem((width, ff), F32), vmem((width, ff), F32), vmem((width, ff), F32),
                vmem((rows_n, width), BF16),
                dma((3,)), dma((micro, CUTS)), dma((micro, CUTS)), dma((2, CUTS)), dma((2, CUTS)),
                dma((CUTS,)), dma((CUTS,)), dma((CUTS,)), dma((2,)), dma((3,)),
            ],
            compiler_params=pltpu.CompilerParams(collective_id=0, has_side_effects=True, vmem_limit_bytes=67_000_000),
            name="pipeline",
        )(x, dy, w_gate, w_up, w_down)
        return g, u, d

    return jax.shard_map(
        step,
        mesh=mesh,
        in_specs=(P("rep", None, None),) * 2 + (P("pp", None, None),) * 3,
        out_specs=(P(("rep", "pp"), None, None),) * 3,
        check_vma=False,
    )
```

```python
import jax
import jax.numpy as jnp
from jax import lax
from jax.experimental import pallas as pl
from jax.experimental.pallas import tpu as pltpu
from jax.sharding import PartitionSpec as P

F32, BF16 = jnp.float32, jnp.bfloat16
CUTS = 4
TILE = 512


def dot(a, b):
    return jnp.dot(a, b, preferred_element_type=F32)


def rounded(x):
    return x.astype(BF16).astype(F32)


def scale_of(wide):
    return lax.rsqrt(jnp.mean(wide * wide, -1, keepdims=True) + 1e-6)


def kernel(x, dy, w_gate, w_up, w_down, out_gate, out_up, out_down, far_act, far_hid,
           wg, wu, wd, wgt, wut, wdt, ahead, behind, send_a, send_b, act, hidden, dgate, dup, at, dyt, tot_g, tot_u, tot_d,
           a_blk, sem_w, sem_a, sem_b, sem_sa, sem_sb, sem_far, sem_near, sem_hfar, sem_hnear, sem_out):
    micro, tokens, width = ahead.shape
    ff = wg.shape[1]
    rows_n = tokens // CUTS
    me, last = lax.axis_index("pp"), lax.axis_size("pp") - 1
    to_go = last - me
    delay = to_go + to_go // 2
    near = delay == 1

    def rows(c):
        return pl.ds(pl.multiple_of(c * rows_n, rows_n), rows_n)

    def each(f):
        pl.loop(0, CUTS)(f)

    def take_x(k, c):
        return pltpu.make_async_copy(x.at[k, rows(c)], ahead.at[k, rows(c)], sem_a.at[k, c])

    def take_dy(k, c):
        return pltpu.make_async_copy(dy.at[k, rows(c)], behind.at[k, rows(c)], sem_b.at[k, c])

    loads = [pltpu.make_async_copy(src.at[0], dst, sem_w.at[i]) for i, (src, dst) in enumerate(((w_gate, wg), (w_up, wu), (w_down, wd)))]

    @pl.when(me == 0)
    def _():
        each(lambda c: take_x(0, c).start())

    for load in loads:
        load.start()

    @pl.when(me == 0)
    def _():
        @pl.loop(1, micro)
        def _(k):
            each(lambda c: take_x(k, c).start())

    @pl.when(me == last)
    def _():
        @pl.loop(0, micro)
        def _(k):
            each(lambda c: take_dy(k, c).start())

    barrier = pltpu.get_barrier_semaphore()

    @pl.when(me > 0)
    def _():
        pl.semaphore_signal(barrier, inc=1, device_id={"pp": me - 1}, device_id_type=pl.DeviceIdType.MESH)

    @pl.when(me < last)
    def _():
        pl.semaphore_signal(barrier, inc=1, device_id={"pp": me + 1}, device_id_type=pl.DeviceIdType.MESH)

    pl.semaphore_wait(barrier, jnp.minimum(me, 1) + jnp.minimum(last - me, 1))

    def pass_on(k, c):
        return pltpu.make_async_remote_copy(
            src_ref=send_a.at[k % 2, rows(c)], dst_ref=ahead.at[k, rows(c)], send_sem=sem_sa.at[k % 2, c], recv_sem=sem_a.at[k, c],
            device_id={"pp": jnp.minimum(me + 1, last)}, device_id_type=pl.DeviceIdType.MESH)

    def pass_back(m, c):
        return pltpu.make_async_remote_copy(
            src_ref=send_b.at[m % 2, rows(c)], dst_ref=behind.at[m, rows(c)], send_sem=sem_sb.at[m % 2, c], recv_sem=sem_b.at[m, c],
            device_id={"pp": jnp.maximum(me - 1, 0)}, device_id_type=pl.DeviceIdType.MESH)

    def slot_f(k):
        return jnp.where(near, k % 2, 0)

    def slot_b(m):
        return jnp.where(near, m % 2, 1)

    def hidden_f(k):
        return jnp.where(near, k % 3, 0)

    def hidden_w(m):
        return jnp.where(near, m % 3, 1 + m % 2)

    def put_away(k, c):
        return (pltpu.make_async_copy(act.at[0, c], far_act.at[k, c], sem_far.at[c]),
                pltpu.make_async_copy(hidden.at[0, rows(c)], far_hid.at[k, rows(c)], sem_hfar.at[c]))

    def fetch(m, c):
        return pltpu.make_async_copy(far_act.at[m, c], act.at[1, c], sem_near.at[c])

    def fetch_hidden(m):
        return pltpu.make_async_copy(far_hid.at[m], hidden.at[1 + m % 2], sem_hnear.at[m % 2])

    def silu_parts(g, u):
        half = 0.5 * g
        z = jnp.tanh(half)
        q = half * z
        return half + q, u * ((0.5 * z + 0.5) * ((half - q) + 1.0))

    def work_forward(k, c):
        slot, slot_h = slot_f(k), hidden_f(k)
        wide = ahead[k, rows(c), :].astype(F32)
        a_blk[...] = (wide * scale_of(wide)).astype(BF16)
        for n in range(0, ff, TILE):
            g = dot(a_blk[...], wg[:, n:n + TILE])
            u = dot(a_blk[...], wu[:, n:n + TILE])
            t, v = silu_parts(g, u)
            act[slot, c, :, n:n + TILE] = t
            act[slot, c, :, ff + n:ff + n + TILE] = v
            hidden[slot_h, rows(c), n:n + TILE] = (t * u).astype(BF16)
        y = rounded(dot(hidden[slot_h, rows(c), :], wd[...]))
        send_a[k % 2, rows(c), :] = (ahead[k, rows(c), :].astype(F32) + y).astype(BF16)

    def by_hidden(m, c):
        slot, keep = slot_b(m), m % 2
        for n in range(0, ff, TILE):
            dh = rounded(dot(behind[m, rows(c), :], wdt[:, n:n + TILE]))
            dup[keep, rows(c), n:n + TILE] = (dh * act[slot, c, :, n:n + TILE]).astype(BF16)
            dgate[keep, rows(c), n:n + TILE] = (dh * act[slot, c, :, ff + n:ff + n + TILE]).astype(BF16)

    def by_input(m, c, keep, send):
        if send:
            da = rounded(rounded(dot(dup[keep, rows(c), :], wut[...])) + rounded(dot(dgate[keep, rows(c), :], wgt[...])))
        wide = ahead[m, rows(c), :].astype(F32)
        scale = scale_of(wide)
        normed = wide * scale
        at[keep, :, rows(c)] = normed.astype(BF16).T
        dyt[keep, :, rows(c)] = behind[m, rows(c), :].T
        if send:
            inner = jnp.sum(da * wide, -1, keepdims=True)
            by_norm = rounded(da * scale + (inner * (scale * scale * scale) * (-1.0 / width)) * wide)
            send_b[m % 2, rows(c), :] = (behind[m, rows(c), :].astype(F32) + by_norm).astype(BF16)

    def work_last(k, c):
        wide = ahead[k, rows(c), :].astype(F32)
        a_blk[...] = (wide * scale_of(wide)).astype(BF16)
        for n in range(0, ff, TILE):
            g = dot(a_blk[...], wg[:, n:n + TILE])
            u = dot(a_blk[...], wu[:, n:n + TILE])
            dh = rounded(dot(behind[k, rows(c), :], wdt[:, n:n + TILE]))
            t, v = silu_parts(g, u)
            hidden[k % 2, rows(c), n:n + TILE] = (t * u).astype(BF16)
            dup[k % 2, rows(c), n:n + TILE] = (dh * t).astype(BF16)
            dgate[k % 2, rows(c), n:n + TILE] = (dh * v).astype(BF16)
        by_input(k, c, k % 2, True)

    def weights(keep, slot):
        for n in range(0, ff, TILE):
            tot_g[:, n:n + TILE] += rounded(dot(at[keep], dgate[keep, :, n:n + TILE]))
            tot_u[:, n:n + TILE] += rounded(dot(at[keep], dup[keep, :, n:n + TILE]))
            tot_d[:, n:n + TILE] += rounded(dot(dyt[keep], hidden[slot, :, n:n + TILE]))

    def weights_part(keep, slot, c):
        part = pl.ds(pl.multiple_of(c * (width // CUTS), width // CUTS), width // CUTS)
        tot_g[part, :] += rounded(dot(at[keep, part, :], dgate[keep]))
        tot_u[part, :] += rounded(dot(at[keep, part, :], dup[keep]))
        tot_d[part, :] += rounded(dot(dyt[keep, part, :], hidden[slot]))

    def before_forward(k, c):
        take_x(k, c).wait()

        @pl.when((k >= 1) & ~near)
        def _():
            for copy in put_away(k - 1, c):
                copy.wait()

        @pl.when(k >= 2)
        def _():
            pass_on(k, c).wait_send()

    def after_forward(k, c):
        pass_on(k, c).start()

        @pl.when(~near)
        def _():
            for copy in put_away(k, c):
                copy.start()

    def before_backward(m, c, send):
        take_dy(m, c).wait()

        @pl.when(~near)
        def _():
            fetch(m, c).wait()

        if send:
            @pl.when(m >= 2)
            def _():
                pass_back(m, c).wait_send()

    def turn():
        wdt[...] = wd[...].T
        wgt[...] = wg[...].T
        wut[...] = wu[...].T

    def clear():
        tot_g[...] = jnp.zeros_like(tot_g)
        tot_u[...] = jnp.zeros_like(tot_u)
        tot_d[...] = jnp.zeros_like(tot_d)

    def run(send):
        @pl.loop(0, micro + delay)
        def _(k):
            m = k - delay

            @pl.when(m < 0)
            def _():
                @each
                def _(c):
                    before_forward(k, c)
                    work_forward(k, c)
                    after_forward(k, c)

            @pl.when((m >= 0) & (m < micro) & ~near)
            def _():
                fetch_hidden(m).start()

            @pl.when((m >= 1) & ~near)
            def _():
                fetch_hidden(m - 1).wait()

            def fetch_next(c):
                @pl.when((m + 1 < micro) & ~near)
                def _():
                    fetch(m + 1, c).start()

            def both(c):
                work_forward(k, c)
                by_hidden(m, c)
                by_input(m, c, m % 2, send)

            def both_sent(c):
                if send:
                    pass_back(m, c).start()
                after_forward(k, c)
                fetch_next(c)

            @pl.when(m == 0)
            def _():
                @each
                def _(c):
                    before_backward(m, c, send)
                    before_forward(k, c)
                    both(c)
                    both_sent(c)

            @pl.when((m >= 1) & (k < micro))
            def _():
                keep, slot = (m - 1) % 2, hidden_w(m - 1)

                @each
                def _(c):
                    take_x(k, c).wait()
                    take_dy(m, c).wait()
                    pass_on(k, c).wait_send()

                    @pl.when(~near)
                    def _():
                        fetch(m, c).wait()
                        for copy in put_away(k - 1, c):
                            copy.wait()

                    if send:
                        @pl.when(m >= 2)
                        def _():
                            pass_back(m, c).wait_send()

                    both(c)
                    weights_part(keep, slot, c)
                    if send:
                        pass_back(m, c).start()
                    pass_on(k, c).start()

                    @pl.when(~near)
                    def _():
                        for copy in put_away(k, c):
                            copy.start()
                        fetch(m + 1, c).start()

            @pl.when((k == micro) & ~near)
            def _():
                @each
                def _(c):
                    for copy in put_away(micro - 1, c):
                        copy.wait()

            @pl.when(k >= micro)
            def _():
                weights((m - 1) % 2, hidden_w(m - 1))

                @each
                def _(c):
                    before_backward(m, c, send)
                    by_hidden(m, c)
                    by_input(m, c, m % 2, send)
                    if send:
                        pass_back(m, c).start()
                    fetch_next(c)

            @pl.when((m == -1) & ~near)
            def _():
                each(lambda c: fetch(0, c).start())

            @pl.when(k == 0)
            def _():
                turn()
                clear()

    for load in loads:
        load.wait()

    @pl.when(me == 0)
    def _():
        run(False)

    @pl.when((me > 0) & (me < last))
    def _():
        run(True)

    @pl.when(me == last)
    def _():
        turn()
        clear()

        def block(k, c, part):
            take_x(k, c).wait()
            take_dy(k, c).wait()

            @pl.when(k >= 2)
            def _():
                pass_back(k, c).wait_send()

            work_last(k, c)
            if part:
                weights_part((k - 1) % 2, (k - 1) % 2, c)
            pass_back(k, c).start()

        each(lambda c: block(0, c, False))

        @pl.loop(1, micro)
        def _(k):
            each(lambda c: block(k, c, True))

    @pl.when((me < last) & ~near)
    def _():
        fetch_hidden(micro - 1).wait()

    keep = (micro - 1) % 2
    spare = 1 - keep
    slot = jnp.where(me == last, keep, hidden_w(micro - 1))
    stores = [pltpu.make_async_copy(src, dst.at[0], sem_out.at[i])
              for i, (src, dst) in enumerate(((dgate.at[spare], out_gate), (dup.at[spare], out_up), (wd, out_down)))]
    for n in range(0, ff, TILE):
        dgate[spare, :, n:n + TILE] = (tot_g[:, n:n + TILE] + rounded(dot(at[keep], dgate[keep, :, n:n + TILE]))).astype(BF16)
    stores[0].start()
    for n in range(0, ff, TILE):
        dup[spare, :, n:n + TILE] = (tot_u[:, n:n + TILE] + rounded(dot(at[keep], dup[keep, :, n:n + TILE]))).astype(BF16)
    stores[1].start()
    for n in range(0, ff, TILE):
        wd[n:n + TILE, :] = (tot_d[:, n:n + TILE] + rounded(dot(dyt[keep], hidden[slot, :, n:n + TILE]))).astype(BF16).T
    stores[2].start()

    @pl.when(me < last)
    def _():
        for k in (micro - 2, micro - 1):
            each(lambda c, k=k: pass_on(k, c).wait_send())

    @pl.when(me > 0)
    def _():
        for m in (micro - 2, micro - 1):
            each(lambda c, m=m: pass_back(m, c).wait_send())

    for store in stores:
        store.wait()


def solution(mesh):
    def step(x, dy, w_gate, w_up, w_down):
        micro, tokens, width = x.shape
        ff = w_gate.shape[2]
        rows_n = tokens // CUTS
        vmem, dma = pltpu.VMEM, pltpu.SemaphoreType.DMA
        any_space = pl.BlockSpec(memory_space=pl.ANY)
        g, u, d, _, _ = pl.pallas_call(
            kernel,
            out_shape=(
                jax.ShapeDtypeStruct((1, width, ff), BF16), jax.ShapeDtypeStruct((1, width, ff), BF16),
                jax.ShapeDtypeStruct((1, ff, width), BF16),
                jax.ShapeDtypeStruct((micro, CUTS, rows_n, 2 * ff), F32), jax.ShapeDtypeStruct((micro, tokens, ff), BF16)),
            in_specs=[any_space] * 5,
            out_specs=(any_space,) * 5,
            scratch_shapes=[
                vmem((width, ff), BF16), vmem((width, ff), BF16), vmem((ff, width), BF16),
                vmem((ff, width), BF16), vmem((ff, width), BF16), vmem((width, ff), BF16),
                vmem(x.shape, BF16), vmem(x.shape, BF16),
                vmem((2, tokens, width), BF16), vmem((2, tokens, width), BF16),
                vmem((2, CUTS, rows_n, 2 * ff), F32), vmem((3, tokens, ff), BF16),
                vmem((2, tokens, ff), BF16), vmem((2, tokens, ff), BF16),
                vmem((2, width, tokens), BF16), vmem((2, width, tokens), BF16),
                vmem((width, ff), F32), vmem((width, ff), F32), vmem((width, ff), F32),
                vmem((rows_n, width), BF16),
                dma((3,)), dma((micro, CUTS)), dma((micro, CUTS)), dma((2, CUTS)), dma((2, CUTS)),
                dma((CUTS,)), dma((CUTS,)), dma((CUTS,)), dma((2,)), dma((3,)),
            ],
            compiler_params=pltpu.CompilerParams(collective_id=0, has_side_effects=True, vmem_limit_bytes=67_000_000),
            name="pipeline",
        )(x, dy, w_gate, w_up, w_down)
        return g, u, d

    return jax.shard_map(
        step,
        mesh=mesh,
        in_specs=(P("rep", None, None),) * 2 + (P("pp", None, None),) * 3,
        out_specs=(P(("rep", "pp"), None, None),) * 3,
        check_vma=False,
    )
```
